128 devices in a mesh: member: 4 (over x, y), gx: 32 (over z, core).
Axes of the slice: x: 2, y: 2, z: 16, core: 2. Of those that a mesh axis runs over, the one named last changes fastest.
The devices are a block of a 8x8x16 slice.
Arguments:
- perturbation: float32 [512, 128, 512], P(('member', 'gx')), parts along dimension 0, may hold values from -6 to 6
- vertical: float32 [512, 128], P('member'), parts along dimension 0, may hold values from -0.5 to 0.5
- kappa: float32 [512, 512], P(('member', 'gx')), parts along dimension 0, may hold values from 2 to 8
- sea_mask: int32 [128, 512], P('gx'), may hold values from 0 to 1
- sweeps: int32 [12], P('member'), parts along dimension 0, may hold values from 4 to 8, as said below
Outputs:
- increment: float32 [512, 128, 512], P('member', 'gx'), parts along dimension 0
The draws below stay inside these ranges and needn't reach their ends.
There are 4 independent parts, one for each index of `member`. The reference program is written for one: setup_inputs(seed, part) draws one part's arguments, and reference() takes and returns one part's arrays. A program takes and returns all parts, laid end to end along the dimension named above; an argument that names none is the same for every part. Nothing has to cross between parts.
Inputs may be any that keep to these rules, and one draw needn't show every extreme that they name: `sweeps`: each entry is at least 4, and one of the three entries equals 8.
All inputs are finite; a program needn't handle non-finite values.
Results may differ from the reference program's by a relative error of at most 0.00007.
Values sent between devices are 32-bit elements; how exact they have to be, the bound alone decides.
A program may use at most 64 MiB of HBM per device.

```python
import math
import jax
import jax.numpy as jnp
from jax import lax

L = 128
NY = 512
SWEEP_MOST = 8
NX = 128


def draw_sweeps(key, part):
    counts = jax.random.randint(key, (3,), 4, SWEEP_MOST + 1).astype(jnp.int32)
    chosen = jax.random.randint(jax.random.fold_in(key, 7), (), 0, 3)
    return jnp.where(jnp.arange(3) == chosen, SWEEP_MOST, counts).astype(jnp.int32)


def draw_sea_mask(key, part):
    walls = jax.random.randint(jax.random.fold_in(key, 11), (1, NY), 0, 2)
    points = jax.random.randint(jax.random.fold_in(key, 13), (NX, NY), 0, 8)
    sea = jnp.where(walls == 1, points == 0, points != 0)
    return sea.astype(jnp.int32)


def levels(own_key, shape, cuts, least, high):
    level = 1.0
    for dim, blocks in cuts:
        heights = jax.random.uniform(jax.random.fold_in(jax.random.fold_in(own_key, 6), dim), (blocks,), jnp.float32, least / len(cuts), high / len(cuts))
        level = level * jnp.repeat(jnp.exp(heights), shape[dim] // blocks).reshape((-1,) + (1,) * (len(shape) - 1 - dim))
    return level


def scatter_about(key, shape, scale, limit, shards=(), dtype=jnp.bfloat16):
    array = jax.random.normal(key, shape, jnp.float32) * scale
    if len(shards) > 0:
        array = levels(key, shape, shards, -0.22, 0.18) * array
    return jnp.clip(array, min=-limit, max=limit).astype(dtype)


def setup_inputs(seed: int = 0, part: int = 0) -> dict:
    streams_of = jax.random.split(jax.random.key(seed), 6)
    own_keys = jax.random.split(jax.random.fold_in(streams_of[5], part), 6)
    return {
        "perturbation": scatter_about(own_keys[0], (L, NX, NY), 1.0, 6.0, ((0, 32),), jnp.float32),
        "vertical": scatter_about(own_keys[1], (L, L), L ** -0.5, 0.5, (), jnp.float32),
        "kappa": jnp.clip(jnp.exp(math.log(8.0) - 1.3862944 * jax.random.uniform(own_keys[2], (NX, NY), jnp.float32) ** levels(own_keys[2], (NX, NY), ((0, 32),), -0.2, 0.2)), 2.0, 8.0),
        "sea_mask": draw_sea_mask(jax.random.fold_in(streams_of[5], 71), part),
        "sweeps": draw_sweeps(jax.random.fold_in(jax.random.fold_in(streams_of[5], part), 71), part),
    }


def couplings(kappa, sea_mask):
    marks = sea_mask.astype(jnp.float32)
    kpad = jnp.pad(kappa, 1)
    mpad = jnp.pad(marks, 1)
    center_k = kpad[1:-1, 1:-1]
    center_m = mpad[1:-1, 1:-1]
    north_side = 0.5 * (center_k + kpad[:-2, 1:-1]) * center_m * mpad[:-2, 1:-1]
    south_side = 0.5 * (center_k + kpad[2:, 1:-1]) * center_m * mpad[2:, 1:-1]
    west_side = 0.5 * (center_k + kpad[1:-1, :-2]) * center_m * mpad[1:-1, :-2]
    east_side = 0.5 * (center_k + kpad[1:-1, 2:]) * center_m * mpad[1:-1, 2:]
    denom = 1.0 + north_side + south_side + west_side + east_side
    return north_side, south_side, west_side, east_side, denom


def reference(perturbation, vertical, kappa, sea_mask, sweeps):
    column = jnp.einsum("lk,kxy->lxy", vertical, perturbation, precision=lax.Precision.HIGHEST)
    north_side, south_side, west_side, east_side, denom = couplings(kappa, sea_mask)
    field = column
    for section in range(3):
        source = field
        count = sweeps[section]

        def sweep(index, iterate):
            padded = jnp.pad(iterate, ((0, 0), (1, 1), (1, 1)))
            gathered = (north_side * padded[:, :-2, 1:-1] + south_side * padded[:, 2:, 1:-1]
                        + west_side * padded[:, 1:-1, :-2] + east_side * padded[:, 1:-1, 2:])
            updated = (source + gathered) / denom
            return jnp.where(index < count, updated, iterate)

        field = lax.fori_loop(0, SWEEP_MOST, sweep, source)
    return field
```

```python
import functools

import jax
import jax.numpy as jnp
from jax import lax
from jax.experimental import pallas as pl
from jax.experimental.pallas import tpu as pltpu
from jax.sharding import PartitionSpec as P

SWEEP_MOST = 8
SWEEP_LEAST = 4
LANES = 128
SUBS = 8
MESH = pl.DeviceIdType.MESH


def kernel(devices, levels, rows, pert, vert, kappa, mask, sweeps, out,
           xin, vin, kin, min_, cnt, kb, coef, u, src, sb, rb, lhs,
           load_sem, one_send, one_recv, two_send, two_recv, swap_send, swap_recv,
           send_sem, recv_sem):
    chips = devices // 2
    steps = rows // SUBS
    blocks = pert.shape[2] // LANES
    own = rows // devices
    slot = own * blocks
    me = lax.axis_index("gx")
    chip = me // 2
    core = lax.rem(me, 2)

    def at(dz, which):
        return lax.rem(chip + dz + chips, chips) * 2 + which

    partner = at(0, 1 - core)
    reach = chips // 4

    barrier = pltpu.get_barrier_semaphore()
    near = [at(s * d, core) for d in range(1, reach + 1) for s in (1, -1)] + [partner]
    for device in near:
        pl.semaphore_signal(barrier, inc=1, device_id={"gx": device}, device_id_type=MESH)

    loads = [
        pltpu.make_async_copy(kappa, kin, load_sem.at[0]),
        pltpu.make_async_copy(mask, min_, load_sem.at[1]),
        pltpu.make_async_copy(sweeps, cnt, load_sem.at[2]),
        pltpu.make_async_copy(vert, vin, load_sem.at[3]),
    ]
    for cb in range(blocks):
        loads.append(pltpu.make_async_copy(
            pert.at[:, :, pl.ds(cb * LANES, LANES)], xin.at[:, cb], load_sem.at[4 + cb]))
    for load in loads:
        load.start()
    loads[0].wait()
    loads[1].wait()
    for cb in range(blocks):
        lanes = pl.ds(cb * LANES, LANES)
        kb[me, pl.ds(cb * own, own), :] = kin[:, lanes] * min_[:, lanes].astype(jnp.float32)

    pl.semaphore_wait(barrier, len(near))

    def give(block, device, ssem, rsem):
        copy = pltpu.make_async_remote_copy(
            src_ref=kb.at[block], dst_ref=kb.at[block], send_sem=ssem, recv_sem=rsem,
            device_id={"gx": device}, device_id_type=MESH)
        copy.start()

    give(me, at(reach, core), one_send, one_recv.at[0])
    give(me, at(-reach, core), one_send, one_recv.at[1])
    for d in range(reach - 1, 0, -1):
        give(me, at(d, core), one_send, one_recv.at[2])
        give(me, at(-d, core), one_send, one_recv.at[2])

    for load in loads[2:]:
        load.wait()
    v = vin[...]
    vh = v.astype(jnp.bfloat16)
    vl = (v - vh.astype(jnp.float32)).astype(jnp.bfloat16)
    depth = lhs.shape[2]
    k_of = lax.broadcasted_iota(jnp.int32, (v.shape[1], depth), 0)
    j_of = lax.broadcasted_iota(jnp.int32, (v.shape[1], depth), 1)
    for c in range(levels):
        pick = k_of == lax.rem(j_of, devices) * levels + c
        high = jnp.where(pick & (j_of < 2 * devices), 1.0, 0.0).astype(jnp.bfloat16)
        low = jnp.where(pick & (j_of >= 2 * devices), 1.0, 0.0).astype(jnp.bfloat16)
        lhs[c] = (jnp.dot(vh, high, preferred_element_type=jnp.float32)
                  + jnp.dot(vl, low, preferred_element_type=jnp.float32)).astype(jnp.bfloat16)

    def arrived(blocks_, sem):
        pltpu.make_async_copy(kb.at[pl.ds(0, blocks_)], kb.at[pl.ds(0, blocks_)], sem).wait()

    arrived(1, one_recv.at[0])
    for d in range(reach, 0, -1):
        give(at(-reach, core), at(d, core), two_send, two_recv)
    arrived(1, one_recv.at[1])
    for d in range(reach - 1, 0, -1):
        give(at(reach, core), at(-d, core), two_send, two_recv)
    arrived(2 * reach - 2, one_recv.at[2])
    arrived(2 * reach - 1, two_recv)

    pairs = kb.reshape(chips, 2, slot, LANES)
    swap = pltpu.make_async_remote_copy(
        src_ref=pairs.at[:, core], dst_ref=pairs.at[:, core], send_sem=swap_send,
        recv_sem=swap_recv, device_id={"gx": partner}, device_id_type=MESH)
    swap.start()
    swap.wait()
    arrived(2 * reach, one_send)
    arrived(2 * reach - 1, two_send)

    kflat = kb.reshape(devices * slot, LANES)
    lane = lax.broadcasted_iota(jnp.int32, (SUBS, LANES), 1)
    sub = lax.broadcasted_iota(jnp.int32, (SUBS, LANES), 0)
    first = lane == 0
    last = lane == LANES - 1
    stride = steps // own * slot

    def place(t, cb):
        return pl.ds(t // own * slot + cb * own + t % own, SUBS, stride=stride)

    def west_of(row, cb, rolled, edge):
        return edge if cb == 0 else jnp.where(first, rolled[cb - 1], rolled[cb])

    def east_of(row, cb, rolled, edge):
        return edge if cb == blocks - 1 else jnp.where(last, rolled[cb + 1], rolled[cb])

    for t in range(steps):
        for cb in range(blocks):
            u[t, cb] = kflat[place(t, cb), :]
    for t in range(steps):
        cur = [u[t, cb] for cb in range(blocks)]
        if t > 0:
            up = [u[t - 1, cb] for cb in range(blocks)]
        else:
            up = [jnp.where(sub == 0, 0.0, pltpu.roll(u[steps - 1, cb], 1, 0)) for cb in range(blocks)]
        if t < steps - 1:
            down = [u[t + 1, cb] for cb in range(blocks)]
        else:
            down = [jnp.where(sub == SUBS - 1, 0.0, pltpu.roll(u[0, cb], SUBS - 1, 0)) for cb in range(blocks)]
        right = [pltpu.roll(c, 1, 1) for c in cur]
        left = [pltpu.roll(c, LANES - 1, 1) for c in cur]
        for cb in range(blocks):
            k = cur[cb]
            half = jnp.where(k > 0.0, 0.5, 0.0)
            sides = []
            for other in (up[cb], down[cb],
                          west_of(cur, cb, right, jnp.where(first, 0.0, right[0])),
                          east_of(cur, cb, left, jnp.where(last, 0.0, left[-1]))):
                sides.append(half * jnp.where(other > 0.0, k + other, 0.0))
            inv = 1.0 / (1.0 + sides[0] + sides[1] + sides[2] + sides[3])
            for i in range(4):
                coef[i, t, cb] = sides[i] * inv
            coef[4, t, cb] = inv

    def sweep(keep):
        top = [u[0, cb] for cb in range(blocks)]
        cur = top
        up = [pltpu.roll(u[steps - 1, cb], 1, 0) for cb in range(blocks)]
        for t in range(steps):
            if t < steps - 1:
                down = [u[t + 1, cb] for cb in range(blocks)]
            else:
                down = [pltpu.roll(c, SUBS - 1, 0) for c in top]
            right = [pltpu.roll(c, 1, 1) for c in cur]
            left = [pltpu.roll(c, LANES - 1, 1) for c in cur]
            for cb in range(blocks):
                new = (src[t, cb] + coef[0, t, cb] * up[cb] + coef[1, t, cb] * down[cb]
                       + (coef[2, t, cb] * west_of(cur, cb, right, right[0])
                          + coef[3, t, cb] * east_of(cur, cb, left, left[-1])))
                if keep is not None:
                    new = jnp.where(keep, new, cur[cb])
                u[t, cb] = new
            up, cur = cur, down

    order = []
    for d in range(chips // 2, 0, -1):
        for s in ((1,) if 2 * d == chips else (1, -1)):
            order += [at(s * d, 1 - core), at(s * d, core)]
    order.append(partner)

    @pl.loop(0, levels)
    def _(l):
        for t in range(steps):
            for cb in range(blocks):
                u[t, cb] = xin[l, cb, pl.ds(t, SUBS, stride=steps), :]

        @pl.loop(0, 3)
        def _(section):
            for t in range(steps):
                for cb in range(blocks):
                    src[t, cb] = u[t, cb] * coef[4, t, cb]
            count = jnp.full((SUBS, LANES), cnt[section], jnp.int32)

            @pl.loop(0, SWEEP_LEAST)
            def _(i):
                sweep(None)

            @pl.loop(SWEEP_LEAST, SWEEP_MOST)
            def _(i):
                sweep(count > i)

        for t in range(steps):
            for cb in range(blocks):
                sb[l, place(t, cb), :] = u[t, cb]
        here = pl.ds(pl.multiple_of(me * slot, slot), slot)
        for device in order:
            pltpu.make_async_remote_copy(
                src_ref=sb.at[l, pl.ds(pl.multiple_of(device * slot, slot), slot)],
                dst_ref=rb.at[l, here], send_sem=send_sem.at[l], recv_sem=recv_sem.at[l],
                device_id={"gx": device}, device_id_type=MESH).start()
        rb[l, here, :] = sb[l, here, :]

    others = pl.ds(0, (devices - 1) * slot)
    width = blocks * LANES

    @pl.loop(0, levels)
    def _(c):
        pltpu.make_async_copy(rb.at[c, others], rb.at[c, others], recv_sem.at[c]).wait()
        left = lhs[c]
        for r in range(own):
            tiles = []
            for cb in range(blocks):
                x = rb[c, pl.ds(cb * own + r, devices, stride=slot), :]
                xh = x.astype(jnp.bfloat16)
                xl = (x - xh.astype(jnp.float32)).astype(jnp.bfloat16)
                tiles.append(jnp.concatenate([xh, xl, xh], axis=0))
            part = jnp.dot(left, jnp.concatenate(tiles, axis=1), preferred_element_type=jnp.float32)
            columns = pl.ds(r * width, width)

            @pl.when(c == 0)
            def _():
                out[:, columns] = part

            @pl.when(c > 0)
            def _():
                out[:, columns] += part

    @pl.loop(0, levels)
    def _(l):
        pltpu.make_async_copy(sb.at[l, others], sb.at[l, others], send_sem.at[l]).wait()


def per_device(perturbation, vertical, kappa, sea_mask, sweeps):
    devices = lax.axis_size("gx")
    levels, rows, columns = perturbation.shape
    own = rows // devices
    blocks = columns // LANES
    steps = rows // SUBS
    slot = own * blocks
    total = vertical.shape[0]
    f32 = jnp.float32
    dma = pltpu.SemaphoreType.DMA
    result = pl.pallas_call(
        functools.partial(kernel, devices, levels, rows),
        out_shape=jax.ShapeDtypeStruct((total, own * columns), f32),
        in_specs=[pl.BlockSpec(memory_space=pl.ANY)] * 5,
        out_specs=pl.BlockSpec(memory_space=pltpu.VMEM),
        scratch_shapes=[
            pltpu.VMEM((levels, blocks, rows, LANES), f32),
            pltpu.VMEM(vertical.shape, f32),
            pltpu.VMEM(kappa.shape, f32),
            pltpu.VMEM(sea_mask.shape, jnp.int32),
            pltpu.SMEM(sweeps.shape, jnp.int32),
            pltpu.VMEM((devices, slot, LANES), f32),
            pltpu.VMEM((5, steps, blocks, SUBS, LANES), f32),
            pltpu.VMEM((steps, blocks, SUBS, LANES), f32),
            pltpu.VMEM((steps, blocks, SUBS, LANES), f32),
            pltpu.VMEM((levels, devices * slot, LANES), f32),
            pltpu.VMEM((levels, devices * slot, LANES), f32),
            pltpu.VMEM((levels, total, 3 * devices), jnp.bfloat16),
            dma((4 + blocks,)),
            dma(()), dma((3,)), dma(()), dma(()), dma(()), dma(()),
            dma((levels,)), dma((levels,)),
        ],
        compiler_params=pltpu.CompilerParams(collective_id=0, has_side_effects=True),
        name="smooth_and_send",
    )(perturbation, vertical, kappa, sea_mask, sweeps)
    return result.reshape(total, own, columns)


def solution(mesh):
    in_specs = (
        P(("member", "gx"), None, None),
        P("member", None),
        P(("member", "gx"), None),
        P("gx", None),
        P("member"),
    )
    out_specs = P("member", "gx", None)
    return jax.shard_map(
        per_device, mesh=mesh, in_specs=in_specs, out_specs=out_specs, check_vma=False
    )
```

```python
import functools

import jax
import jax.numpy as jnp
from jax import lax
from jax.experimental import pallas as pl
from jax.experimental.pallas import tpu as pltpu
from jax.sharding import PartitionSpec as P

SWEEP_MOST = 8
SWEEP_LEAST = 4
LANES = 128
SUBS = 8
MESH = pl.DeviceIdType.MESH


def kernel(devices, levels, rows, pert, vert, kappa, mask, sweeps, out,
           xin, vin, kin, min_, cnt, kb, coef, xi, src, sb, rb, lhs,
           load_sem, one_send, one_recv, two_send, two_recv, send_sem, recv_sem):
    chips = devices // 2
    steps = rows // SUBS
    blocks = pert.shape[2] // LANES
    own = rows // devices
    slot = own * blocks
    me = lax.axis_index("gx")
    chip = me // 2
    core = lax.rem(me, 2)

    def at(dz, which):
        return lax.rem(chip + dz + chips, chips) * 2 + which

    partner = at(0, 1 - core)
    reach = chips // 4

    lane = lax.broadcasted_iota(jnp.int32, (SUBS, LANES), 1)
    sub = lax.broadcasted_iota(jnp.int32, (SUBS, LANES), 0)
    group = LANES // blocks
    low64 = lane < LANES // 2
    low32 = lax.rem(lane, LANES // 2) < group

    def transposed(v):
        a = [None] * 4
        for i in (0, 1):
            a[i] = jnp.where(low64, v[i], pltpu.roll(v[i + 2], LANES // 2, 1))
            a[i + 2] = jnp.where(low64, pltpu.roll(v[i], LANES // 2, 1), v[i + 2])
        b = [None] * 4
        for i in (0, 2):
            b[i] = jnp.where(low32, a[i], pltpu.roll(a[i + 1], group, 1))
            b[i + 1] = jnp.where(low32, pltpu.roll(a[i], LANES - group, 1), a[i + 1])
        return b

    def picked(v, index):
        return [jnp.take_along_axis(x, index, axis=1, mode="promise_in_bounds") for x in v]

    def interleaved(v):
        return transposed(picked(v, lax.rem(lane, group) * blocks + lane // group))

    def natural(v):
        return picked(transposed(v), lax.rem(lane, blocks) * group + lane // blocks)

    barrier = pltpu.get_barrier_semaphore()
    near = [at(s * d, c) for d in range(1, reach + 1) for s in (1, -1) for c in (core, 1 - core)] + [partner]
    for device in near:
        pl.semaphore_signal(barrier, inc=1, device_id={"gx": device}, device_id_type=MESH)

    loads = [
        pltpu.make_async_copy(kappa, kin, load_sem.at[0]),
        pltpu.make_async_copy(mask, min_, load_sem.at[1]),
        pltpu.make_async_copy(sweeps, cnt, load_sem.at[2]),
        pltpu.make_async_copy(vert, vin, load_sem.at[3]),
    ]
    for cb in range(blocks):
        loads.append(pltpu.make_async_copy(
            pert.at[:, :, pl.ds(cb * LANES, LANES)], xin.at[:, cb], load_sem.at[4 + cb]))
    for load in loads:
        load.start()
    loads[0].wait()
    loads[1].wait()
    wet = []
    for cb in range(blocks):
        lanes = pl.ds(cb * LANES, LANES)
        x = kin[:, lanes] * min_[:, lanes].astype(jnp.float32)
        wet.append(jnp.concatenate([x, jnp.zeros((SUBS - own, LANES), jnp.float32)], axis=0))
    for cb, x in enumerate(interleaved(wet)):
        kb[me, pl.ds(cb * own, own), :] = x[:own]

    pl.semaphore_wait(barrier, len(near))

    def give(block, device, ssem, rsem):
        copy = pltpu.make_async_remote_copy(
            src_ref=kb.at[block], dst_ref=kb.at[block], send_sem=ssem, recv_sem=rsem,
            device_id={"gx": device}, device_id_type=MESH)
        copy.start()

    give(me, at(reach, core), one_send, one_recv.at[0])
    give(me, at(-reach, core), one_send, one_recv.at[1])
    give(me, at(reach, 1 - core), one_send, one_recv.at[2])
    give(me, at(-reach, 1 - core), one_send, one_recv.at[2])
    for d in range(reach - 1, 0, -1):
        for c in (core, 1 - core):
            give(me, at(d, c), one_send, one_recv.at[2])
            give(me, at(-d, c), one_send, one_recv.at[2])
    give(me, partner, one_send, one_recv.at[2])

    for load in loads[2:]:
        load.wait()
    v = vin[...]
    vh = v.astype(jnp.bfloat16)
    vl = (v - vh.astype(jnp.float32)).astype(jnp.bfloat16)
    depth = lhs.shape[2]
    k_of = lax.broadcasted_iota(jnp.int32, (v.shape[1], depth), 0)
    j_of = lax.broadcasted_iota(jnp.int32, (v.shape[1], depth), 1)
    for c in range(levels):
        pick = k_of == lax.rem(j_of, devices) * levels + c
        high = jnp.where(pick & (j_of < 2 * devices), 1.0, 0.0).astype(jnp.bfloat16)
        low = jnp.where(pick & (j_of >= 2 * devices), 1.0, 0.0).astype(jnp.bfloat16)
        lhs[c] = (jnp.dot(vh, high, preferred_element_type=jnp.float32)
                  + jnp.dot(vl, low, preferred_element_type=jnp.float32)).astype(jnp.bfloat16)

    def arrived(blocks_, sem):
        pltpu.make_async_copy(kb.at[pl.ds(0, blocks_)], kb.at[pl.ds(0, blocks_)], sem).wait()

    arrived(1, one_recv.at[0])
    for d in range(reach, 0, -1):
        for c in (core, 1 - core):
            give(at(-reach, core), at(d, c), two_send, two_recv)
    arrived(1, one_recv.at[1])
    for d in range(reach - 1, 0, -1):
        for c in (core, 1 - core):
            give(at(reach, core), at(-d, c), two_send, two_recv)

    @pl.loop(0, levels)
    def _(l):
        for t in range(steps):
            v = [xin[l, cb, pl.ds(t, SUBS, stride=steps), :] for cb in range(blocks)]
            for cb, x in enumerate(interleaved(v)):
                xi[l, t, cb] = x

    arrived(4 * reach - 1, one_recv.at[2])
    arrived(4 * reach - 2, two_recv)
    arrived(4 * reach + 1, one_send)
    arrived(4 * reach - 2, two_send)

    kflat = kb.reshape(devices * slot, LANES)
    first = lane == 0
    last = lane == LANES - 1
    stride = steps // own * slot

    def place(t, cb):
        return pl.ds(t // own * slot + cb * own + t % own, SUBS, stride=stride)

    ks = src
    for t in range(steps):
        for cb in range(blocks):
            ks[t, cb] = kflat[place(t, cb), :]
    for t in range(steps):
        cur = [ks[t, cb] for cb in range(blocks)]
        if t > 0:
            up = [ks[t - 1, cb] for cb in range(blocks)]
        else:
            up = [jnp.where(sub == 0, 0.0, pltpu.roll(ks[steps - 1, cb], 1, 0)) for cb in range(blocks)]
        if t < steps - 1:
            down = [ks[t + 1, cb] for cb in range(blocks)]
        else:
            down = [jnp.where(sub == SUBS - 1, 0.0, pltpu.roll(ks[0, cb], SUBS - 1, 0)) for cb in range(blocks)]
        west = [jnp.where(first, 0.0, pltpu.roll(cur[-1], 1, 1))] + cur[:-1]
        east = cur[1:] + [jnp.where(last, 0.0, pltpu.roll(cur[0], LANES - 1, 1))]
        for cb in range(blocks):
            k = cur[cb]
            half = jnp.where(k > 0.0, 0.5, 0.0)
            sides = []
            for other in (up[cb], down[cb], west[cb], east[cb]):
                sides.append(half * jnp.where(other > 0.0, k + other, 0.0))
            inv = 1.0 / (1.0 + sides[0] + sides[1] + sides[2] + sides[3])
            for i in range(4):
                coef[i, t, cb] = sides[i] * inv
            coef[4, t, cb] = inv

    def sweep(u, keep):
        top = [u[0, cb] for cb in range(blocks)]
        cur = top
        up = [pltpu.roll(u[steps - 1, cb], 1, 0) for cb in range(blocks)]
        for t in range(steps):
            if t < steps - 1:
                down = [u[t + 1, cb] for cb in range(blocks)]
            else:
                down = [pltpu.roll(c, SUBS - 1, 0) for c in top]
            west = [pltpu.roll(cur[-1], 1, 1)] + cur[:-1]
            east = cur[1:] + [pltpu.roll(cur[0], LANES - 1, 1)]
            for cb in range(blocks):
                new = (src[t, cb] + coef[0, t, cb] * up[cb] + coef[1, t, cb] * down[cb]
                       + (coef[2, t, cb] * west[cb] + coef[3, t, cb] * east[cb]))
                if keep is not None:
                    new = jnp.where(keep, new, cur[cb])
                u[t, cb] = new
            up, cur = cur, down

    order = []
    for d in range(chips // 2, 0, -1):
        for s in ((1,) if 2 * d == chips else (1, -1)):
            order += [at(s * d, 1 - core), at(s * d, core)]
    order.append(partner)

    @pl.loop(0, levels)
    def _(l):
        u = xi.at[l]

        @pl.loop(0, 3)
        def _(section):
            for t in range(steps):
                for cb in range(blocks):
                    src[t, cb] = u[t, cb] * coef[4, t, cb]
            count = jnp.full((SUBS, LANES), cnt[section], jnp.int32)

            @pl.loop(0, SWEEP_LEAST)
            def _(i):
                sweep(u, None)

            @pl.loop(SWEEP_LEAST, SWEEP_MOST)
            def _(i):
                sweep(u, count > i)

        for t in range(steps):
            for cb, x in enumerate(natural([u[t, cb] for cb in range(blocks)])):
                sb[l, place(t, cb), :] = x
        here = pl.ds(pl.multiple_of(me * slot, slot), slot)
        for device in order:
            pltpu.make_async_remote_copy(
                src_ref=sb.at[l, pl.ds(pl.multiple_of(device * slot, slot), slot)],
                dst_ref=rb.at[l, here], send_sem=send_sem.at[l], recv_sem=recv_sem.at[l],
                device_id={"gx": device}, device_id_type=MESH).start()
        rb[l, here, :] = sb[l, here, :]

    others = pl.ds(0, (devices - 1) * slot)
    width = blocks * LANES

    @pl.loop(0, levels)
    def _(c):
        pltpu.make_async_copy(rb.at[c, others], rb.at[c, others], recv_sem.at[c]).wait()
        left = lhs[c]
        for r in range(own):
            tiles = []
            for cb in range(blocks):
                x = rb[c, pl.ds(cb * own + r, devices, stride=slot), :]
                xh = x.astype(jnp.bfloat16)
                xl = (x - xh.astype(jnp.float32)).astype(jnp.bfloat16)
                tiles.append(jnp.concatenate([xh, xl, xh], axis=0))
            part = jnp.dot(left, jnp.concatenate(tiles, axis=1), preferred_element_type=jnp.float32)
            columns = pl.ds(r * width, width)

            @pl.when(c == 0)
            def _():
                out[:, columns] = part

            @pl.when(c > 0)
            def _():
                out[:, columns] += part

    @pl.loop(0, levels)
    def _(l):
        pltpu.make_async_copy(sb.at[l, others], sb.at[l, others], send_sem.at[l]).wait()


def per_device(perturbation, vertical, kappa, sea_mask, sweeps):
    devices = lax.axis_size("gx")
    levels, rows, columns = perturbation.shape
    own = rows // devices
    blocks = columns // LANES
    steps = rows // SUBS
    slot = own * blocks
    total = vertical.shape[0]
    f32 = jnp.float32
    dma = pltpu.SemaphoreType.DMA
    result = pl.pallas_call(
        functools.partial(kernel, devices, levels, rows),
        out_shape=jax.ShapeDtypeStruct((total, own * columns), f32),
        in_specs=[pl.BlockSpec(memory_space=pl.ANY)] * 5,
        out_specs=pl.BlockSpec(memory_space=pltpu.VMEM),
        scratch_shapes=[
            pltpu.VMEM((levels, blocks, rows, LANES), f32),
            pltpu.VMEM(vertical.shape, f32),
            pltpu.VMEM(kappa.shape, f32),
            pltpu.VMEM(sea_mask.shape, jnp.int32),
            pltpu.SMEM(sweeps.shape, jnp.int32),
            pltpu.VMEM((devices, slot, LANES), f32),
            pltpu.VMEM((5, steps, blocks, SUBS, LANES), f32),
            pltpu.VMEM((levels, steps, blocks, SUBS, LANES), f32),
            pltpu.VMEM((steps, blocks, SUBS, LANES), f32),
            pltpu.VMEM((levels, devices * slot, LANES), f32),
            pltpu.VMEM((levels, devices * slot, LANES), f32),
            pltpu.VMEM((levels, total, 3 * devices), jnp.bfloat16),
            dma((4 + blocks,)),
            dma(()), dma((3,)), dma(()), dma(()),
            dma((levels,)), dma((levels,)),
        ],
        compiler_params=pltpu.CompilerParams(collective_id=0, has_side_effects=True),
        name="smooth_and_send",
    )(perturbation, vertical, kappa, sea_mask, sweeps)
    return result.reshape(total, own, columns)


def solution(mesh):
    in_specs = (
        P(("member", "gx"), None, None),
        P("member", None),
        P(("member", "gx"), None),
        P("gx", None),
        P("member"),
    )
    out_specs = P("member", "gx", None)
    return jax.shard_map(
        per_device, mesh=mesh, in_specs=in_specs, out_specs=out_specs, check_vma=False
    )
```

```python
import functools

import jax
import jax.numpy as jnp
from jax import lax
from jax.experimental import pallas as pl
from jax.experimental.pallas import tpu as pltpu
from jax.sharding import PartitionSpec as P

SWEEP_MOST = 8
SWEEP_LEAST = 4
LANES = 128
SUBS = 8
MESH = pl.DeviceIdType.MESH


def kernel(devices, levels, rows, pert, vert, kappa, mask, sweeps, out,
           xin, vin, kin, min_, cnt, kb, coef, xi, src, sb, rb, lhs,
           load_sem, one_send, one_recv, two_send, two_recv, send_sem, recv_sem):
    chips = devices // 2
    steps = rows // SUBS
    blocks = pert.shape[2] // LANES
    own = rows // devices
    slot = own * blocks
    me = lax.axis_index("gx")
    chip = me // 2
    core = lax.rem(me, 2)

    def at(dz, which):
        return lax.rem(me + 2 * (dz + chips), devices) - core + which

    partner = at(0, 1 - core)
    reach = chips // 4

    lane = lax.broadcasted_iota(jnp.int32, (SUBS, LANES), 1)
    sub = lax.broadcasted_iota(jnp.int32, (SUBS, LANES), 0)
    group = LANES // blocks
    low64 = lane < LANES // 2
    low32 = lax.rem(lane, LANES // 2) < group

    def transposed(v):
        a = [None] * 4
        for i in (0, 1):
            a[i] = jnp.where(low64, v[i], pltpu.roll(v[i + 2], LANES // 2, 1))
            a[i + 2] = jnp.where(low64, pltpu.roll(v[i], LANES // 2, 1), v[i + 2])
        b = [None] * 4
        for i in (0, 2):
            b[i] = jnp.where(low32, a[i], pltpu.roll(a[i + 1], group, 1))
            b[i + 1] = jnp.where(low32, pltpu.roll(a[i], LANES - group, 1), a[i + 1])
        return b

    def picked(v, index):
        return [jnp.take_along_axis(x, index, axis=1, mode="promise_in_bounds") for x in v]

    def interleaved(v):
        return transposed(picked(v, lax.rem(lane, group) * blocks + lane // group))

    def natural(v):
        return picked(transposed(v), lax.rem(lane, blocks) * group + lane // blocks)

    barrier = pltpu.get_barrier_semaphore()
    loads = [
        pltpu.make_async_copy(kappa, kin, load_sem.at[0]),
        pltpu.make_async_copy(mask, min_, load_sem.at[1]),
        pltpu.make_async_copy(sweeps, cnt, load_sem.at[2]),
        pltpu.make_async_copy(vert, vin, load_sem.at[3]),
    ]
    for cb in range(blocks):
        loads.append(pltpu.make_async_copy(
            pert.at[:, :, pl.ds(cb * LANES, LANES)], xin.at[:, cb], load_sem.at[4 + cb]))
    for load in loads[:2]:
        load.start()
    near = [at(s * d, c) for d in range(1, reach + 1) for s in (1, -1) for c in (core, 1 - core)] + [partner]
    for device in near:
        pl.semaphore_signal(barrier, inc=1, device_id={"gx": device}, device_id_type=MESH)

    for load in loads[2:]:
        load.start()
    loads[0].wait()
    loads[1].wait()
    wet = []
    for cb in range(blocks):
        lanes = pl.ds(cb * LANES, LANES)
        x = kin[:, lanes] * min_[:, lanes].astype(jnp.float32)
        wet.append(jnp.concatenate([x, jnp.zeros((SUBS - own, LANES), jnp.float32)], axis=0))
    for cb, x in enumerate(interleaved(wet)):
        kb[me, pl.ds(cb * own, own), :] = x[:own]

    pl.semaphore_wait(barrier, len(near))

    def give(block, device, ssem, rsem):
        copy = pltpu.make_async_remote_copy(
            src_ref=kb.at[block], dst_ref=kb.at[block], send_sem=ssem, recv_sem=rsem,
            device_id={"gx": device}, device_id_type=MESH)
        copy.start()

    give(me, at(reach, core), one_send, one_recv.at[0])
    give(me, at(-reach, core), one_send, one_recv.at[1])
    give(me, at(reach, 1 - core), one_send, one_recv.at[2])
    give(me, at(-reach, 1 - core), one_send, one_recv.at[2])
    for d in range(reach - 1, 0, -1):
        for c in (core, 1 - core):
            give(me, at(d, c), one_send, one_recv.at[2])
            give(me, at(-d, c), one_send, one_recv.at[2])
    give(me, partner, one_send, one_recv.at[2])

    for load in loads[2:]:
        load.wait()
    v = vin[...]
    vh = v.astype(jnp.bfloat16)
    vl = (v - vh.astype(jnp.float32)).astype(jnp.bfloat16)
    depth = lhs.shape[2]
    k_of = lax.broadcasted_iota(jnp.int32, (v.shape[1], depth), 0)
    j_of = lax.broadcasted_iota(jnp.int32, (v.shape[1], depth), 1)
    for c in range(levels):
        pick = k_of == lax.rem(j_of, devices) * levels + c
        high = jnp.where(pick & (j_of < 2 * devices), 1.0, 0.0).astype(jnp.bfloat16)
        low = jnp.where(pick & (j_of >= 2 * devices), 1.0, 0.0).astype(jnp.bfloat16)
        lhs[c] = (jnp.dot(vh, high, preferred_element_type=jnp.float32)
                  + jnp.dot(vl, low, preferred_element_type=jnp.float32)).astype(jnp.bfloat16)

    def arrived(blocks_, sem):
        pltpu.make_async_copy(kb.at[pl.ds(0, blocks_)], kb.at[pl.ds(0, blocks_)], sem).wait()

    arrived(1, one_recv.at[0])
    for d in range(reach, 0, -1):
        for c in (core, 1 - core):
            give(at(-reach, core), at(d, c), two_send, two_recv)
    arrived(1, one_recv.at[1])
    for d in range(reach - 1, 0, -1):
        for c in (core, 1 - core):
            give(at(reach, core), at(-d, c), two_send, two_recv)

    @pl.loop(0, levels)
    def _(l):
        for t in range(steps):
            v = [xin[l, cb, pl.ds(t, SUBS, stride=steps), :] for cb in range(blocks)]
            for cb, x in enumerate(interleaved(v)):
                xi[l, t, cb] = x

    arrived(4 * reach - 1, one_recv.at[2])
    arrived(4 * reach - 2, two_recv)
    arrived(4 * reach + 1, one_send)
    arrived(4 * reach - 2, two_send)

    kflat = kb.reshape(devices * slot, LANES)
    first = lane == 0
    last = lane == LANES - 1
    stride = steps // own * slot

    def place(t, cb):
        return pl.ds(t // own * slot + cb * own + t % own, SUBS, stride=stride)

    ks = src
    for t in range(steps):
        for cb in range(blocks):
            ks[t, cb] = kflat[place(t, cb), :]
    for t in range(steps):
        cur = [ks[t, cb] for cb in range(blocks)]
        if t > 0:
            up = [ks[t - 1, cb] for cb in range(blocks)]
        else:
            up = [jnp.where(sub == 0, 0.0, pltpu.roll(ks[steps - 1, cb], 1, 0)) for cb in range(blocks)]
        if t < steps - 1:
            down = [ks[t + 1, cb] for cb in range(blocks)]
        else:
            down = [jnp.where(sub == SUBS - 1, 0.0, pltpu.roll(ks[0, cb], SUBS - 1, 0)) for cb in range(blocks)]
        west = [jnp.where(first, 0.0, pltpu.roll(cur[-1], 1, 1))] + cur[:-1]
        east = cur[1:] + [jnp.where(last, 0.0, pltpu.roll(cur[0], LANES - 1, 1))]
        for cb in range(blocks):
            k = cur[cb]
            half = jnp.where(k > 0.0, 0.5, 0.0)
            sides = []
            for other in (up[cb], down[cb], west[cb], east[cb]):
                sides.append(half * jnp.where(other > 0.0, k + other, 0.0))
            inv = 1.0 / (1.0 + sides[0] + sides[1] + sides[2] + sides[3])
            for i in range(4):
                coef[i, t, cb] = sides[i] * inv
            coef[4, t, cb] = inv

    def sweep(u, keep):
        top = [u[0, cb] for cb in range(blocks)]
        cur = top
        up = [pltpu.roll(u[steps - 1, cb], 1, 0) for cb in range(blocks)]
        for t in range(steps):
            if t < steps - 1:
                down = [u[t + 1, cb] for cb in range(blocks)]
            else:
                down = [pltpu.roll(c, SUBS - 1, 0) for c in top]
            west = [pltpu.roll(cur[-1], 1, 1)] + cur[:-1]
            east = cur[1:] + [pltpu.roll(cur[0], LANES - 1, 1)]
            for cb in range(blocks):
                new = (src[t, cb] + coef[0, t, cb] * up[cb] + coef[1, t, cb] * down[cb]
                       + (coef[2, t, cb] * west[cb] + coef[3, t, cb] * east[cb]))
                if keep is not None:
                    new = jnp.where(keep, new, cur[cb])
                u[t, cb] = new
            up, cur = cur, down

    here = pl.ds(pl.multiple_of(me * slot, slot), slot)
    early = devices // 4

    def post(l, wanted):
        for j in wanted:
            device = jnp.where(me == j, devices - 1, j)
            pltpu.make_async_remote_copy(
                src_ref=sb.at[l, pl.ds(pl.multiple_of(device * slot, slot), slot)],
                dst_ref=rb.at[l, here], send_sem=send_sem.at[l], recv_sem=recv_sem.at[l],
                device_id={"gx": device}, device_id_type=MESH).start()

    @pl.loop(0, levels)
    def _(l):
        u = xi.at[l]

        @pl.loop(0, 3)
        def _(section):
            for t in range(steps):
                for cb in range(blocks):
                    src[t, cb] = u[t, cb] * coef[4, t, cb]
            count = jnp.full((SUBS, LANES), cnt[section], jnp.int32)

            @pl.loop(0, SWEEP_LEAST)
            def _(i):
                sweep(u, None)

            @pl.loop(SWEEP_LEAST, SWEEP_MOST)
            def _(i):
                sweep(u, count > i)

        for t in range(steps):
            for cb, x in enumerate(natural([u[t, cb] for cb in range(blocks)])):
                sb[l, place(t, cb), :] = x
        post(l, range(early))

        @pl.when(l == 0)
        def _():
            post(l, range(early, devices - 1))

        rb[l, here, :] = sb[l, here, :]

    @pl.loop(1, levels)
    def _(l):
        post(l, range(early, devices - 1))

    others = pl.ds(0, (devices - 1) * slot)
    width = blocks * LANES

    @pl.loop(0, levels)
    def _(c):
        pltpu.make_async_copy(rb.at[c, others], rb.at[c, others], recv_sem.at[c]).wait()
        left = lhs[c]
        for r in range(own):
            tiles = []
            for cb in range(blocks):
                x = rb[c, pl.ds(cb * own + r, devices, stride=slot), :]
                xh = x.astype(jnp.bfloat16)
                xl = (x - xh.astype(jnp.float32)).astype(jnp.bfloat16)
                tiles.append(jnp.concatenate([xh, xl, xh], axis=0))
            part = jnp.dot(left, jnp.concatenate(tiles, axis=1), preferred_element_type=jnp.float32)
            columns = pl.ds(r * width, width)

            @pl.when(c == 0)
            def _():
                out[:, columns] = part

            @pl.when(c > 0)
            def _():
                out[:, columns] += part

    @pl.loop(0, levels)
    def _(l):
        pltpu.make_async_copy(sb.at[l, others], sb.at[l, others], send_sem.at[l]).wait()


def per_device(perturbation, vertical, kappa, sea_mask, sweeps):
    devices = lax.axis_size("gx")
    levels, rows, columns = perturbation.shape
    own = rows // devices
    blocks = columns // LANES
    steps = rows // SUBS
    slot = own * blocks
    total = vertical.shape[0]
    f32 = jnp.float32
    dma = pltpu.SemaphoreType.DMA
    result = pl.pallas_call(
        functools.partial(kernel, devices, levels, rows),
        out_shape=pltpu.VMEM((total, own * columns), f32),
        in_specs=[pl.BlockSpec(memory_space=pl.ANY)] * 5,
        out_specs=pl.BlockSpec(memory_space=pltpu.VMEM),
        scratch_shapes=[
            pltpu.VMEM((levels, blocks, rows, LANES), f32),
            pltpu.VMEM(vertical.shape, f32),
            pltpu.VMEM(kappa.shape, f32),
            pltpu.VMEM(sea_mask.shape, jnp.int32),
            pltpu.SMEM(sweeps.shape, jnp.int32),
            pltpu.VMEM((devices, slot, LANES), f32),
            pltpu.VMEM((5, steps, blocks, SUBS, LANES), f32),
            pltpu.VMEM((levels, steps, blocks, SUBS, LANES), f32),
            pltpu.VMEM((steps, blocks, SUBS, LANES), f32),
            pltpu.VMEM((levels, devices * slot, LANES), f32),
            pltpu.VMEM((levels, devices * slot, LANES), f32),
            pltpu.VMEM((levels, total, 3 * devices), jnp.bfloat16),
            dma((4 + blocks,)),
            dma(()), dma((3,)), dma(()), dma(()),
            dma((levels,)), dma((levels,)),
        ],
        compiler_params=pltpu.CompilerParams(collective_id=0, has_side_effects=True),
        name="smooth_and_send",
    )(perturbation, vertical, kappa, sea_mask, sweeps)
    return result.reshape(total, own, columns)


def solution(mesh):
    in_specs = (
        P(("member", "gx"), None, None),
        P("member", None),
        P(("member", "gx"), None),
        P("gx", None),
        P("member"),
    )
    out_specs = P("member", "gx", None)
    return jax.shard_map(
        per_device, mesh=mesh, in_specs=in_specs, out_specs=out_specs, check_vma=False
    )
```

```python
import functools

import jax
import jax.numpy as jnp
from jax import lax
from jax.experimental import pallas as pl
from jax.experimental.pallas import tpu as pltpu
from jax.sharding import PartitionSpec as P

SWEEP_MOST = 8
SWEEP_LEAST = 4
LANES = 128
SUBS = 8
MESH = pl.DeviceIdType.MESH


def kernel(devices, levels, rows, pert, vert, kappa, mask, sweeps, out,
           xin, vin, kin, min_, cnt, kb, coef, xi, src, sb, rb, lhs, acc,
           load_sem, one_send, two_send, block_recv, send_sem, recv_sem):
    chips = devices // 2
    steps = rows // SUBS
    blocks = pert.shape[2] // LANES
    own = rows // devices
    slot = own * blocks
    me = lax.axis_index("gx")
    chip = me // 2
    core = lax.rem(me, 2)

    def at(dz, which):
        return lax.rem(me + 2 * (dz + chips), devices) - core + which

    partner = at(0, 1 - core)
    reach = chips // 4

    lane = lax.broadcasted_iota(jnp.int32, (SUBS, LANES), 1)
    sub = lax.broadcasted_iota(jnp.int32, (SUBS, LANES), 0)
    group = LANES // blocks
    low64 = lane < LANES // 2
    low32 = lax.rem(lane, LANES // 2) < group

    def transposed(v):
        a = [None] * 4
        for i in (0, 1):
            a[i] = jnp.where(low64, v[i], pltpu.roll(v[i + 2], LANES // 2, 1))
            a[i + 2] = jnp.where(low64, pltpu.roll(v[i], LANES // 2, 1), v[i + 2])
        b = [None] * 4
        for i in (0, 2):
            b[i] = jnp.where(low32, a[i], pltpu.roll(a[i + 1], group, 1))
            b[i + 1] = jnp.where(low32, pltpu.roll(a[i], LANES - group, 1), a[i + 1])
        return b

    def picked(v, index):
        return [jnp.take_along_axis(x, index, axis=1, mode="promise_in_bounds") for x in v]

    def interleaved(v):
        return transposed(picked(v, lax.rem(lane, group) * blocks + lane // group))

    def natural(v):
        return picked(transposed(v), lax.rem(lane, blocks) * group + lane // blocks)

    barrier = pltpu.get_barrier_semaphore()
    loads = [
        pltpu.make_async_copy(kappa, kin, load_sem.at[0]),
        pltpu.make_async_copy(mask, min_, load_sem.at[1]),
        pltpu.make_async_copy(sweeps, cnt, load_sem.at[2]),
        pltpu.make_async_copy(vert, vin, load_sem.at[3]),
    ]
    for cb in range(blocks):
        loads.append(pltpu.make_async_copy(
            pert.at[:, :, pl.ds(cb * LANES, LANES)], xin.at[:, cb], load_sem.at[4 + cb]))
    for load in loads[:2]:
        load.start()
    near = [at(s * d, c) for d in range(1, reach + 1) for s in (1, -1) for c in (core, 1 - core)] + [partner]
    for device in near:
        pl.semaphore_signal(barrier, inc=1, device_id={"gx": device}, device_id_type=MESH)

    for load in loads[2:]:
        load.start()
    loads[0].wait()
    loads[1].wait()
    wet = []
    for cb in range(blocks):
        lanes = pl.ds(cb * LANES, LANES)
        x = kin[:, lanes] * min_[:, lanes].astype(jnp.float32)
        wet.append(jnp.concatenate([x, jnp.zeros((SUBS - own, LANES), jnp.float32)], axis=0))
    for cb, x in enumerate(interleaved(wet)):
        kb[me, pl.ds(cb * own, own), :] = x[:own]

    pl.semaphore_wait(barrier, len(near))

    def give(block, device, ssem):
        pltpu.make_async_remote_copy(
            src_ref=kb.at[block], dst_ref=kb.at[block], send_sem=ssem,
            recv_sem=block_recv.at[block],
            device_id={"gx": device}, device_id_type=MESH).start()

    for d in range(reach, 0, -1):
        for c in (core, 1 - core):
            give(me, at(d, c), one_send)
            give(me, at(-d, c), one_send)
    give(me, partner, one_send)

    for load in loads[2:]:
        load.wait()
    v = vin[...]
    vh = v.astype(jnp.bfloat16)
    vl = (v - vh.astype(jnp.float32)).astype(jnp.bfloat16)
    depth = lhs.shape[2]
    k_of = lax.broadcasted_iota(jnp.int32, (v.shape[1], depth), 0)
    j_of = lax.broadcasted_iota(jnp.int32, (v.shape[1], depth), 1)
    for c in range(levels):
        pick = k_of == lax.rem(j_of, devices) * levels + c
        high = jnp.where(pick & (j_of < 2 * devices), 1.0, 0.0).astype(jnp.bfloat16)
        low = jnp.where(pick & (j_of >= 2 * devices), 1.0, 0.0).astype(jnp.bfloat16)
        lhs[c] = (jnp.dot(vh, high, preferred_element_type=jnp.float32)
                  + jnp.dot(vl, low, preferred_element_type=jnp.float32)).astype(jnp.bfloat16)

    def sent(blocks_, sem):
        pltpu.make_async_copy(kb.at[pl.ds(0, blocks_)], kb.at[pl.ds(0, blocks_)], sem).wait()

    def arrived(block):
        pltpu.make_async_copy(kb.at[block], kb.at[block], block_recv.at[block]).wait()

    below, above = at(-reach, core), at(reach, core)
    arrived(below)
    for d in range(reach, 0, -1):
        for c in (core, 1 - core):
            give(below, at(d, c), two_send)
    arrived(above)
    for d in range(reach - 1, 0, -1):
        for c in (core, 1 - core):
            give(above, at(-d, c), two_send)

    def others_arrived(start, stop):
        @pl.loop(start, stop)
        def _(j):
            @pl.when((j != me) & (j != below) & (j != above))
            def _():
                arrived(j)

    @pl.loop(0, levels)
    def _(l):
        for t in range(steps):
            v = [xin[l, cb, pl.ds(t, SUBS, stride=steps), :] for cb in range(blocks)]
            for cb, x in enumerate(interleaved(v)):
                xi[l, t, cb] = x

    kflat = kb.reshape(devices * slot, LANES)
    first = lane == 0
    last = lane == LANES - 1

    def place(t, cb, count):
        return pl.ds(t // own * slot + cb * own + t % own, SUBS, stride=count // own * slot)

    def couple(count):
        ks = src
        for t in range(count):
            for cb in range(blocks):
                ks[t, cb] = kflat[place(t, cb, count), :]
        for t in range(count):
            cur = [ks[t, cb] for cb in range(blocks)]
            if t > 0:
                up = [ks[t - 1, cb] for cb in range(blocks)]
            else:
                up = [jnp.where(sub == 0, 0.0, pltpu.roll(ks[count - 1, cb], 1, 0)) for cb in range(blocks)]
            if t < count - 1:
                down = [ks[t + 1, cb] for cb in range(blocks)]
            else:
                down = [jnp.where(sub == SUBS - 1, 0.0, pltpu.roll(ks[0, cb], SUBS - 1, 0)) for cb in range(blocks)]
            west = [jnp.where(first, 0.0, pltpu.roll(cur[-1], 1, 1))] + cur[:-1]
            east = cur[1:] + [jnp.where(last, 0.0, pltpu.roll(cur[0], LANES - 1, 1))]
            for cb in range(blocks):
                k = cur[cb]
                half = jnp.where(k > 0.0, 0.5, 0.0)
                sides = []
                for other in (up[cb], down[cb], west[cb], east[cb]):
                    sides.append(half * jnp.where(other > 0.0, k + other, 0.0))
                inv = 1.0 / (1.0 + sides[0] + sides[1] + sides[2] + sides[3])
                for i in range(4):
                    coef[i, t, cb] = sides[i] * inv
                coef[4, t, cb] = inv

    def sweep(u, count, start, keep):
        def row(t):
            return [u[t % count, cb] for cb in range(blocks)]

        top = row(start)
        up, cur = row(start - 1), top
        for i in range(count):
            t = (start + i) % count
            down = row(t + 1) if i < count - 1 else top
            north = [pltpu.roll(c, 1, 0) for c in up] if t == 0 else up
            south = [pltpu.roll(c, SUBS - 1, 0) for c in down] if t == count - 1 else down
            west = [pltpu.roll(cur[-1], 1, 1)] + cur[:-1]
            east = cur[1:] + [pltpu.roll(cur[0], LANES - 1, 1)]
            for cb in range(blocks):
                new = (src[t, cb] + coef[0, t, cb] * north[cb] + coef[1, t, cb] * south[cb]
                       + (coef[2, t, cb] * west[cb] + coef[3, t, cb] * east[cb]))
                if keep is not None:
                    new = jnp.where(keep, new, cur[cb])
                u[t, cb] = new
            up, cur = cur, down

    def diffuse(u, count, to):
        @pl.loop(0, 3)
        def _(section):
            for t in range(count):
                for cb in range(blocks):
                    src[t, cb] = u[t, cb] * coef[4, t, cb]
            most = jnp.full((SUBS, LANES), cnt[section], jnp.int32)

            @pl.loop(0, SWEEP_LEAST, step=2)
            def _(i):
                sweep(u, count, 0, None)
                sweep(u, count, 2, None)

            @pl.loop(SWEEP_LEAST, SWEEP_MOST, step=2)
            def _(i):
                sweep(u, count, 0, most > i)
                sweep(u, count, 2, most > i + 1)

        for t in range(count):
            for cb, x in enumerate(natural([u[t, cb] for cb in range(blocks)])):
                to[place(t, cb, count), :] = x

    here = pl.ds(pl.multiple_of(me * slot, slot), slot)
    early = devices // 4

    def send(l, rows_, device):
        pltpu.make_async_remote_copy(
            src_ref=rows_.at[pl.ds(pl.multiple_of(device * slot, slot), slot)],
            dst_ref=rb.at[l, here], send_sem=send_sem.at[l], recv_sem=recv_sem.at[l],
            device_id={"gx": device}, device_id_type=MESH).start()

    def post(l, wanted):
        for j in wanted:
            send(l, sb.at[l], jnp.where(me == j, devices - 1, j))

    others_arrived(0, devices)
    couple(steps)

    @pl.loop(0, levels)
    def _(l):
        diffuse(xi.at[l], steps, sb.at[l])

        post(l, range(early))

        @pl.when(l == 0)
        def _():
            post(l, range(early, devices - 1))

        rb[l, here, :] = sb[l, here, :]

    @pl.loop(1, levels)
    def _(l):
        post(l, range(early, devices - 1))

    others = pl.ds(0, (devices - 1) * slot)
    width = blocks * LANES

    @pl.loop(0, levels)
    def _(c):
        pltpu.make_async_copy(rb.at[c, others], rb.at[c, others], recv_sem.at[c]).wait()
        left = lhs[c]
        for r in range(own):
            tiles = []
            for cb in range(blocks):
                x = rb[c, pl.ds(cb * own + r, devices, stride=slot), :]
                xh = x.astype(jnp.bfloat16)
                xl = (x - xh.astype(jnp.float32)).astype(jnp.bfloat16)
                tiles.append(jnp.concatenate([xh, xl, xh], axis=0))
            part = jnp.dot(left, jnp.concatenate(tiles, axis=1), preferred_element_type=jnp.float32)
            columns = pl.ds(r * width, width)

            @pl.when(c == 0)
            def _():
                acc[:, columns] = part

            @pl.when((c > 0) & (c < levels - 1))
            def _():
                acc[:, columns] += part

            @pl.when(c == levels - 1)
            def _():
                out[:, r, :] = acc[:, columns] + part

    @pl.loop(0, levels)
    def _(l):
        pltpu.make_async_copy(sb.at[l, others], sb.at[l, others], send_sem.at[l]).wait()

    sent(4 * reach + 1, one_send)
    sent(4 * reach - 2, two_send)


def per_device(perturbation, vertical, kappa, sea_mask, sweeps):
    devices = lax.axis_size("gx")
    levels, rows, columns = perturbation.shape
    own = rows // devices
    blocks = columns // LANES
    steps = rows // SUBS
    slot = own * blocks
    total = vertical.shape[0]
    f32 = jnp.float32
    dma = pltpu.SemaphoreType.DMA
    result = pl.pallas_call(
        functools.partial(kernel, devices, levels, rows),
        out_shape=pltpu.VMEM((total, own, columns), f32),
        in_specs=[pl.BlockSpec(memory_space=pl.ANY)] * 5,
        out_specs=pl.BlockSpec(memory_space=pltpu.VMEM),
        scratch_shapes=[
            pltpu.VMEM((levels, blocks, rows, LANES), f32),
            pltpu.VMEM(vertical.shape, f32),
            pltpu.VMEM(kappa.shape, f32),
            pltpu.VMEM(sea_mask.shape, jnp.int32),
            pltpu.SMEM(sweeps.shape, jnp.int32),
            pltpu.VMEM((devices, slot, LANES), f32),
            pltpu.VMEM((5, steps, blocks, SUBS, LANES), f32),
            pltpu.VMEM((levels, steps, blocks, SUBS, LANES), f32),
            pltpu.VMEM((steps, blocks, SUBS, LANES), f32),
            pltpu.VMEM((levels, devices * slot, LANES), f32),
            pltpu.VMEM((levels, devices * slot, LANES), f32),
            pltpu.VMEM((levels, total, 3 * devices), jnp.bfloat16),
            pltpu.VMEM((total, own * columns), f32),
            dma((4 + blocks,)),
            dma(()), dma(()), dma((devices,)),
            dma((levels,)), dma((levels,)),
        ],
        compiler_params=pltpu.CompilerParams(collective_id=0, has_side_effects=True),
        name="smooth_and_send",
    )(perturbation, vertical, kappa, sea_mask, sweeps)
    return result


def solution(mesh):
    in_specs = (
        P(("member", "gx"), None, None),
        P("member", None),
        P(("member", "gx"), None),
        P("gx", None),
        P("member"),
    )
    out_specs = P("member", "gx", None)
    return jax.shard_map(
        per_device, mesh=mesh, in_specs=in_specs, out_specs=out_specs, check_vma=False
    )
```

```python
import functools

import jax
import jax.numpy as jnp
from jax import lax
from jax.experimental import pallas as pl
from jax.experimental.pallas import tpu as pltpu
from jax.sharding import PartitionSpec as P

SWEEP_MOST = 8
SWEEP_LEAST = 4
LANES = 128
SUBS = 8
MESH = pl.DeviceIdType.MESH


def kernel(devices, levels, rows, pert, vert, kappa, mask, sweeps, out,
           xin, vin, kin, min_, cnt, kb, coef, xi, src, sb, rb, lhs, acc,
           load_sem, one_send, one_recv, two_send, two_recv, send_sem, recv_sem):
    chips = devices // 2
    steps = rows // SUBS
    blocks = pert.shape[2] // LANES
    own = rows // devices
    slot = own * blocks
    me = lax.axis_index("gx")
    chip = me // 2
    core = lax.rem(me, 2)

    def at(dz, which):
        return lax.rem(me + 2 * (dz + chips), devices) - core + which

    partner = at(0, 1 - core)
    reach = chips // 4

    lane = lax.broadcasted_iota(jnp.int32, (SUBS, LANES), 1)
    sub = lax.broadcasted_iota(jnp.int32, (SUBS, LANES), 0)
    group = LANES // blocks
    low64 = lane < LANES // 2
    low32 = lax.rem(lane, LANES // 2) < group

    def transposed(v):
        a = [None] * 4
        for i in (0, 1):
            a[i] = jnp.where(low64, v[i], pltpu.roll(v[i + 2], LANES // 2, 1))
            a[i + 2] = jnp.where(low64, pltpu.roll(v[i], LANES // 2, 1), v[i + 2])
        b = [None] * 4
        for i in (0, 2):
            b[i] = jnp.where(low32, a[i], pltpu.roll(a[i + 1], group, 1))
            b[i + 1] = jnp.where(low32, pltpu.roll(a[i], LANES - group, 1), a[i + 1])
        return b

    def picked(v, index):
        return [jnp.take_along_axis(x, index, axis=1, mode="promise_in_bounds") for x in v]

    def interleaved(v):
        return transposed(picked(v, lax.rem(lane, group) * blocks + lane // group))

    def natural(v):
        return picked(transposed(v), lax.rem(lane, blocks) * group + lane // blocks)

    barrier = pltpu.get_barrier_semaphore()
    loads = [
        pltpu.make_async_copy(kappa, kin, load_sem.at[0]),
        pltpu.make_async_copy(mask, min_, load_sem.at[1]),
        pltpu.make_async_copy(sweeps, cnt, load_sem.at[2]),
        pltpu.make_async_copy(vert, vin, load_sem.at[3]),
    ]
    for cb in range(blocks):
        loads.append(pltpu.make_async_copy(
            pert.at[:, :, pl.ds(cb * LANES, LANES)], xin.at[:, cb], load_sem.at[4 + cb]))
    for load in loads[:2]:
        load.start()
    near = [at(s * d, c) for d in range(reach, 0, -1) for s in (1, -1) for c in (core, 1 - core)] + [partner]
    for device in near:
        pl.semaphore_signal(barrier, inc=1, device_id={"gx": device}, device_id_type=MESH)

    for load in loads[2:]:
        load.start()
    loads[0].wait()
    loads[1].wait()
    wet = []
    for cb in range(blocks):
        lanes = pl.ds(cb * LANES, LANES)
        x = kin[:, lanes] * min_[:, lanes].astype(jnp.float32)
        wet.append(jnp.concatenate([x, jnp.zeros((SUBS - own, LANES), jnp.float32)], axis=0))
    for cb, x in enumerate(interleaved(wet)):
        kb[me, pl.ds(cb * own, own), :] = x[:own]

    pl.semaphore_wait(barrier, len(near))

    def give(block, device, ssem, rsem):
        copy = pltpu.make_async_remote_copy(
            src_ref=kb.at[block], dst_ref=kb.at[block], send_sem=ssem, recv_sem=rsem,
            device_id={"gx": device}, device_id_type=MESH)
        copy.start()

    give(me, at(reach, core), one_send, one_recv.at[0])
    give(me, at(-reach, core), one_send, one_recv.at[1])
    give(me, at(reach, 1 - core), one_send, one_recv.at[2])
    give(me, at(-reach, 1 - core), one_send, one_recv.at[2])
    for d in range(reach - 1, 0, -1):
        for c in (core, 1 - core):
            give(me, at(d, c), one_send, one_recv.at[2])
            give(me, at(-d, c), one_send, one_recv.at[2])
    give(me, partner, one_send, one_recv.at[2])

    for load in loads[2:]:
        load.wait()
    v = vin[...]
    vh = v.astype(jnp.bfloat16)
    vl = (v - vh.astype(jnp.float32)).astype(jnp.bfloat16)
    depth = lhs.shape[2]
    k_of = lax.broadcasted_iota(jnp.int32, (v.shape[1], depth), 0)
    j_of = lax.broadcasted_iota(jnp.int32, (v.shape[1], depth), 1)
    for c in range(levels):
        pick = k_of == lax.rem(j_of, devices) * levels + c
        high = jnp.where(pick & (j_of < 2 * devices), 1.0, 0.0).astype(jnp.bfloat16)
        low = jnp.where(pick & (j_of >= 2 * devices), 1.0, 0.0).astype(jnp.bfloat16)
        lhs[c] = (jnp.dot(vh, high, preferred_element_type=jnp.float32)
                  + jnp.dot(vl, low, preferred_element_type=jnp.float32)).astype(jnp.bfloat16)

    def arrived(blocks_, sem):
        pltpu.make_async_copy(kb.at[pl.ds(0, blocks_)], kb.at[pl.ds(0, blocks_)], sem).wait()

    arrived(1, one_recv.at[0])
    for d in range(reach, 0, -1):
        for c in (core, 1 - core):
            give(at(-reach, core), at(d, c), two_send, two_recv)
    arrived(1, one_recv.at[1])
    for d in range(reach - 1, 0, -1):
        for c in (core, 1 - core):
            give(at(reach, core), at(-d, c), two_send, two_recv)

    @pl.loop(0, levels)
    def _(l):
        for t in range(steps):
            v = [xin[l, cb, pl.ds(t, SUBS, stride=steps), :] for cb in range(blocks)]
            for cb, x in enumerate(interleaved(v)):
                xi[l, t, cb] = x

    kflat = kb.reshape(devices * slot, LANES)
    first = lane == 0
    last = lane == LANES - 1

    def place(t, cb, count):
        return pl.ds(t // own * slot + cb * own + t % own, SUBS, stride=count // own * slot)

    def couple(count):
        ks = src
        for t in range(count):
            for cb in range(blocks):
                ks[t, cb] = kflat[place(t, cb, count), :]
        for t in range(count):
            cur = [ks[t, cb] for cb in range(blocks)]
            if t > 0:
                up = [ks[t - 1, cb] for cb in range(blocks)]
            else:
                up = [jnp.where(sub == 0, 0.0, pltpu.roll(ks[count - 1, cb], 1, 0)) for cb in range(blocks)]
            if t < count - 1:
                down = [ks[t + 1, cb] for cb in range(blocks)]
            else:
                down = [jnp.where(sub == SUBS - 1, 0.0, pltpu.roll(ks[0, cb], SUBS - 1, 0)) for cb in range(blocks)]
            west = [jnp.where(first, 0.0, pltpu.roll(cur[-1], 1, 1))] + cur[:-1]
            east = cur[1:] + [jnp.where(last, 0.0, pltpu.roll(cur[0], LANES - 1, 1))]
            for cb in range(blocks):
                k = cur[cb]
                half = jnp.where(k > 0.0, 0.5, 0.0)
                sides = []
                for other in (up[cb], down[cb], west[cb], east[cb]):
                    sides.append(half * jnp.where(other > 0.0, k + other, 0.0))
                inv = 1.0 / (1.0 + sides[0] + sides[1] + sides[2] + sides[3])
                for i in range(4):
                    coef[i, t, cb] = sides[i] * inv
                coef[4, t, cb] = inv

    def sweep(u, count, start, keep):
        def row(t):
            return [u[t % count, cb] for cb in range(blocks)]

        top = row(start)
        up, cur = row(start - 1), top
        for i in range(count):
            t = (start + i) % count
            down = row(t + 1) if i < count - 1 else top
            north = [pltpu.roll(c, 1, 0) for c in up] if t == 0 else up
            south = [pltpu.roll(c, SUBS - 1, 0) for c in down] if t == count - 1 else down
            west = [pltpu.roll(cur[-1], 1, 1)] + cur[:-1]
            east = cur[1:] + [pltpu.roll(cur[0], LANES - 1, 1)]
            for cb in range(blocks):
                new = (src[t, cb] + coef[0, t, cb] * north[cb] + coef[1, t, cb] * south[cb]
                       + (coef[2, t, cb] * west[cb] + coef[3, t, cb] * east[cb]))
                if keep is not None:
                    new = jnp.where(keep, new, cur[cb])
                u[t, cb] = new
            up, cur = cur, down

    def diffuse(u, count, to):
        @pl.loop(0, 3)
        def _(section):
            for t in range(count):
                for cb in range(blocks):
                    src[t, cb] = u[t, cb] * coef[4, t, cb]
            most = jnp.full((SUBS, LANES), cnt[section], jnp.int32)

            @pl.loop(0, SWEEP_LEAST, step=2)
            def _(i):
                sweep(u, count, 0, None)
                sweep(u, count, 2, None)

            @pl.loop(SWEEP_LEAST, SWEEP_MOST, step=2)
            def _(i):
                sweep(u, count, 0, most > i)
                sweep(u, count, 2, most > i + 1)

        for t in range(count):
            for cb, x in enumerate(natural([u[t, cb] for cb in range(blocks)])):
                to[place(t, cb, count), :] = x

    here = pl.ds(pl.multiple_of(me * slot, slot), slot)
    early = devices // 4

    def send(l, rows_, device):
        pltpu.make_async_remote_copy(
            src_ref=rows_.at[pl.ds(pl.multiple_of(device * slot, slot), slot)],
            dst_ref=rb.at[l, here], send_sem=send_sem.at[l], recv_sem=recv_sem.at[l],
            device_id={"gx": device}, device_id_type=MESH).start()

    def post(l, wanted):
        for j in wanted:
            send(l, sb.at[l], jnp.where(me == j, devices - 1, j))

    arrived(4 * reach - 1, one_recv.at[2])
    arrived(4 * reach - 2, two_recv)
    couple(steps)

    @pl.loop(0, levels)
    def _(l):
        diffuse(xi.at[l], steps, sb.at[l])

        post(l, range(early))

        @pl.when(l == 0)
        def _():
            post(l, range(early, devices - 1))

        rb[l, here, :] = sb[l, here, :]

    @pl.loop(1, levels)
    def _(l):
        post(l, range(early, devices - 1))

    others = pl.ds(0, (devices - 1) * slot)
    width = blocks * LANES

    @pl.loop(0, levels)
    def _(c):
        pltpu.make_async_copy(rb.at[c, others], rb.at[c, others], recv_sem.at[c]).wait()
        left = lhs[c]
        for r in range(own):
            tiles = []
            for cb in range(blocks):
                x = rb[c, pl.ds(cb * own + r, devices, stride=slot), :]
                xh = x.astype(jnp.bfloat16)
                xl = (x - xh.astype(jnp.float32)).astype(jnp.bfloat16)
                tiles.append(jnp.concatenate([xh, xl, xh], axis=0))
            part = jnp.dot(left, jnp.concatenate(tiles, axis=1), preferred_element_type=jnp.float32)
            columns = pl.ds(r * width, width)

            @pl.when(c == 0)
            def _():
                acc[:, columns] = part

            @pl.when((c > 0) & (c < levels - 1))
            def _():
                acc[:, columns] += part

            @pl.when(c == levels - 1)
            def _():
                out[:, r, :] = acc[:, columns] + part

    @pl.loop(0, levels)
    def _(l):
        pltpu.make_async_copy(sb.at[l, others], sb.at[l, others], send_sem.at[l]).wait()

    arrived(4 * reach + 1, one_send)
    arrived(4 * reach - 2, two_send)


def per_device(perturbation, vertical, kappa, sea_mask, sweeps):
    devices = lax.axis_size("gx")
    levels, rows, columns = perturbation.shape
    own = rows // devices
    blocks = columns // LANES
    steps = rows // SUBS
    slot = own * blocks
    total = vertical.shape[0]
    f32 = jnp.float32
    dma = pltpu.SemaphoreType.DMA
    result = pl.pallas_call(
        functools.partial(kernel, devices, levels, rows),
        out_shape=pltpu.VMEM((total, own, columns), f32),
        in_specs=[pl.BlockSpec(memory_space=pl.ANY)] * 5,
        out_specs=pl.BlockSpec(memory_space=pltpu.VMEM),
        scratch_shapes=[
            pltpu.VMEM((levels, blocks, rows, LANES), f32),
            pltpu.VMEM(vertical.shape, f32),
            pltpu.VMEM(kappa.shape, f32),
            pltpu.VMEM(sea_mask.shape, jnp.int32),
            pltpu.SMEM(sweeps.shape, jnp.int32),
            pltpu.VMEM((devices, slot, LANES), f32),
            pltpu.VMEM((5, steps, blocks, SUBS, LANES), f32),
            pltpu.VMEM((levels, steps, blocks, SUBS, LANES), f32),
            pltpu.VMEM((steps, blocks, SUBS, LANES), f32),
            pltpu.VMEM((levels, devices * slot, LANES), f32),
            pltpu.VMEM((levels, devices * slot, LANES), f32),
            pltpu.VMEM((levels, total, 3 * devices), jnp.bfloat16),
            pltpu.VMEM((total, own * columns), f32),
            dma((4 + blocks,)),
            dma(()), dma((3,)), dma(()), dma(()),
            dma((levels,)), dma((levels,)),
        ],
        compiler_params=pltpu.CompilerParams(collective_id=0, has_side_effects=True),
        name="smooth_and_send",
    )(perturbation, vertical, kappa, sea_mask, sweeps)
    return result


def solution(mesh):
    in_specs = (
        P(("member", "gx"), None, None),
        P("member", None),
        P(("member", "gx"), None),
        P("gx", None),
        P("member"),
    )
    out_specs = P("member", "gx", None)
    return jax.shard_map(
        per_device, mesh=mesh, in_specs=in_specs, out_specs=out_specs, check_vma=False
    )
```

```python
import functools

import jax
import jax.numpy as jnp
from jax import lax
from jax.experimental import pallas as pl
from jax.experimental.pallas import tpu as pltpu
from jax.sharding import PartitionSpec as P

SWEEP_MOST = 8
SWEEP_LEAST = 4
LANES = 128
SUBS = 8
MESH = pl.DeviceIdType.MESH


def kernel(devices, levels, rows, pert, vert, kappa, mask, sweeps, out,
           xin, vin, kin, min_, cnt, kb, coef, xi, src, sb, rb, lhs, acc,
           load_sem, one_send, one_recv, two_send, two_recv, send_sem, recv_sem):
    chips = devices // 2
    steps = rows // SUBS
    blocks = pert.shape[2] // LANES
    own = rows // devices
    slot = own * blocks
    me = lax.axis_index("gx")
    chip = me // 2
    core = lax.rem(me, 2)

    def at(dz, which):
        return lax.rem(me + 2 * (dz + chips), devices) - core + which

    partner = at(0, 1 - core)
    reach = chips // 4

    lane = lax.broadcasted_iota(jnp.int32, (SUBS, LANES), 1)
    sub = lax.broadcasted_iota(jnp.int32, (SUBS, LANES), 0)
    group = LANES // blocks
    low64 = lane < LANES // 2
    low32 = lax.rem(lane, LANES // 2) < group

    def transposed(v):
        a = [None] * 4
        for i in (0, 1):
            a[i] = jnp.where(low64, v[i], pltpu.roll(v[i + 2], LANES // 2, 1))
            a[i + 2] = jnp.where(low64, pltpu.roll(v[i], LANES // 2, 1), v[i + 2])
        b = [None] * 4
        for i in (0, 2):
            b[i] = jnp.where(low32, a[i], pltpu.roll(a[i + 1], group, 1))
            b[i + 1] = jnp.where(low32, pltpu.roll(a[i], LANES - group, 1), a[i + 1])
        return b

    def picked(v, index):
        return [jnp.take_along_axis(x, index, axis=1, mode="promise_in_bounds") for x in v]

    def interleaved(v):
        return transposed(picked(v, lax.rem(lane, group) * blocks + lane // group))

    def natural(v):
        return picked(transposed(v), lax.rem(lane, blocks) * group + lane // blocks)

    barrier = pltpu.get_barrier_semaphore()
    loads = [
        pltpu.make_async_copy(kappa, kin, load_sem.at[0]),
        pltpu.make_async_copy(mask, min_, load_sem.at[1]),
        pltpu.make_async_copy(sweeps, cnt, load_sem.at[2]),
        pltpu.make_async_copy(vert, vin, load_sem.at[3]),
    ]
    for cb in range(blocks):
        loads.append(pltpu.make_async_copy(
            pert.at[:, :, pl.ds(cb * LANES, LANES)], xin.at[:, cb], load_sem.at[4 + cb]))
    for load in loads[:2]:
        load.start()
    near = [at(s * d, c) for d in range(reach, 0, -1) for s in (1, -1) for c in (core, 1 - core)] + [partner]
    for device in near:
        pl.semaphore_signal(barrier, inc=1, device_id={"gx": device}, device_id_type=MESH)

    for load in loads[2:]:
        load.start()
    loads[0].wait()
    loads[1].wait()
    wet = []
    for cb in range(blocks):
        lanes = pl.ds(cb * LANES, LANES)
        x = kin[:, lanes] * min_[:, lanes].astype(jnp.float32)
        wet.append(jnp.concatenate([x, jnp.zeros((SUBS - own, LANES), jnp.float32)], axis=0))
    for cb, x in enumerate(interleaved(wet)):
        kb[me, pl.ds(cb * own, own), :] = x[:own]

    pl.semaphore_wait(barrier, len(near))

    def give(block, device, ssem, rsem):
        copy = pltpu.make_async_remote_copy(
            src_ref=kb.at[block], dst_ref=kb.at[block], send_sem=ssem, recv_sem=rsem,
            device_id={"gx": device}, device_id_type=MESH)
        copy.start()

    give(me, at(reach, core), one_send, one_recv.at[0])
    give(me, at(-reach, core), one_send, one_recv.at[1])
    give(me, at(reach, 1 - core), one_send, one_recv.at[2])
    give(me, at(-reach, 1 - core), one_send, one_recv.at[2])
    for d in range(reach - 1, 0, -1):
        for c in (core, 1 - core):
            give(me, at(d, c), one_send, one_recv.at[2])
            give(me, at(-d, c), one_send, one_recv.at[2])
    give(me, partner, one_send, one_recv.at[2])

    for load in loads[2:]:
        load.wait()
    v = vin[...]
    vh = v.astype(jnp.bfloat16)
    vl = (v - vh.astype(jnp.float32)).astype(jnp.bfloat16)
    depth = lhs.shape[2]
    k_of = lax.broadcasted_iota(jnp.int32, (v.shape[1], depth), 0)
    j_of = lax.broadcasted_iota(jnp.int32, (v.shape[1], depth), 1)
    for c in range(levels):
        pick = k_of == lax.rem(j_of, devices) * levels + c
        high = jnp.where(pick & (j_of < 2 * devices), 1.0, 0.0).astype(jnp.bfloat16)
        low = jnp.where(pick & (j_of >= 2 * devices), 1.0, 0.0).astype(jnp.bfloat16)
        lhs[c] = (jnp.dot(vh, high, preferred_element_type=jnp.float32)
                  + jnp.dot(vl, low, preferred_element_type=jnp.float32)).astype(jnp.bfloat16)

    def arrived(blocks_, sem):
        pltpu.make_async_copy(kb.at[pl.ds(0, blocks_)], kb.at[pl.ds(0, blocks_)], sem).wait()

    arrived(1, one_recv.at[0])
    for d in range(reach, 0, -1):
        for c in (core, 1 - core):
            give(at(-reach, core), at(d, c), two_send, two_recv)
    arrived(1, one_recv.at[1])
    for d in range(reach - 1, 0, -1):
        for c in (core, 1 - core):
            give(at(reach, core), at(-d, c), two_send, two_recv)

    @pl.loop(0, levels)
    def _(l):
        for t in range(steps):
            v = [xin[l, cb, pl.ds(t, SUBS, stride=steps), :] for cb in range(blocks)]
            for cb, x in enumerate(interleaved(v)):
                xi[l, t, cb] = x

    kflat = kb.reshape(devices * slot, LANES)
    first = lane == 0
    last = lane == LANES - 1

    def place(t, cb, count):
        return pl.ds(t // own * slot + cb * own + t % own, SUBS, stride=count // own * slot)

    def couple(count):
        ks = src
        for t in range(count):
            for cb in range(blocks):
                ks[t, cb] = kflat[place(t, cb, count), :]
        for t in range(count):
            cur = [ks[t, cb] for cb in range(blocks)]
            if t > 0:
                up = [ks[t - 1, cb] for cb in range(blocks)]
            else:
                up = [jnp.where(sub == 0, 0.0, pltpu.roll(ks[count - 1, cb], 1, 0)) for cb in range(blocks)]
            if t < count - 1:
                down = [ks[t + 1, cb] for cb in range(blocks)]
            else:
                down = [jnp.where(sub == SUBS - 1, 0.0, pltpu.roll(ks[0, cb], SUBS - 1, 0)) for cb in range(blocks)]
            west = [jnp.where(first, 0.0, pltpu.roll(cur[-1], 1, 1))] + cur[:-1]
            east = cur[1:] + [jnp.where(last, 0.0, pltpu.roll(cur[0], LANES - 1, 1))]
            for cb in range(blocks):
                k = cur[cb]
                half = jnp.where(k > 0.0, 0.5, 0.0)
                sides = []
                for other in (up[cb], down[cb], west[cb], east[cb]):
                    sides.append(half * jnp.where(other > 0.0, k + other, 0.0))
                inv = 1.0 / (1.0 + sides[0] + sides[1] + sides[2] + sides[3])
                for i in range(4):
                    coef[i, t, cb] = sides[i] * inv
                coef[4, t, cb] = inv

    def sweep(u, count, start, keep):
        def row(t):
            return [u[t % count, cb] for cb in range(blocks)]

        top = row(start)
        up, cur = row(start - 1), top
        for i in range(count):
            t = (start + i) % count
            down = row(t + 1) if i < count - 1 else top
            north = [pltpu.roll(c, 1, 0) for c in up] if t == 0 else up
            south = [pltpu.roll(c, SUBS - 1, 0) for c in down] if t == count - 1 else down
            west = [pltpu.roll(cur[-1], 1, 1)] + cur[:-1]
            east = cur[1:] + [pltpu.roll(cur[0], LANES - 1, 1)]
            for cb in range(blocks):
                new = (src[t, cb] + coef[0, t, cb] * north[cb] + coef[1, t, cb] * south[cb]
                       + (coef[2, t, cb] * west[cb] + coef[3, t, cb] * east[cb]))
                if keep is not None:
                    new = jnp.where(keep, new, cur[cb])
                u[t, cb] = new
            up, cur = cur, down

    def diffuse(u, count, to):
        @pl.loop(0, 3)
        def _(section):
            for t in range(count):
                for cb in range(blocks):
                    src[t, cb] = u[t, cb] * coef[4, t, cb]
            most = jnp.full((SUBS, LANES), cnt[section], jnp.int32)

            for i in range(SWEEP_LEAST):
                sweep(u, count, 2 * i, None)

            @pl.loop(SWEEP_LEAST, SWEEP_MOST, step=2)
            def _(i):
                sweep(u, count, 0, most > i)
                sweep(u, count, 2, most > i + 1)

        for t in range(count):
            for cb, x in enumerate(natural([u[t, cb] for cb in range(blocks)])):
                to[place(t, cb, count), :] = x

    here = pl.ds(pl.multiple_of(me * slot, slot), slot)
    early = devices // 4

    def send(l, rows_, device):
        pltpu.make_async_remote_copy(
            src_ref=rows_.at[pl.ds(pl.multiple_of(device * slot, slot), slot)],
            dst_ref=rb.at[l, here], send_sem=send_sem.at[l], recv_sem=recv_sem.at[l],
            device_id={"gx": device}, device_id_type=MESH).start()

    def post(l, wanted):
        for j in wanted:
            send(l, sb.at[l], jnp.where(me == j, devices - 1, j))

    arrived(4 * reach - 1, one_recv.at[2])
    arrived(4 * reach - 2, two_recv)
    couple(steps)

    @pl.loop(0, levels)
    def _(l):
        diffuse(xi.at[l], steps, sb.at[l])

        post(l, range(early))

        @pl.when(l == 0)
        def _():
            post(l, range(early, devices - 1))

        rb[l, here, :] = sb[l, here, :]

    @pl.loop(1, levels)
    def _(l):
        post(l, range(early, devices - 1))

    others = pl.ds(0, (devices - 1) * slot)
    width = blocks * LANES

    @pl.loop(0, levels)
    def _(c):
        pltpu.make_async_copy(rb.at[c, others], rb.at[c, others], recv_sem.at[c]).wait()
        left = lhs[c]
        for r in range(own):
            tiles = []
            for cb in range(blocks):
                x = rb[c, pl.ds(cb * own + r, devices, stride=slot), :]
                xh = x.astype(jnp.bfloat16)
                xl = (x - xh.astype(jnp.float32)).astype(jnp.bfloat16)
                tiles.append(jnp.concatenate([xh, xl, xh], axis=0))
            part = jnp.dot(left, jnp.concatenate(tiles, axis=1), preferred_element_type=jnp.float32)
            columns = pl.ds(r * width, width)

            @pl.when(c == 0)
            def _():
                acc[:, columns] = part

            @pl.when((c > 0) & (c < levels - 1))
            def _():
                acc[:, columns] += part

            @pl.when(c == levels - 1)
            def _():
                out[:, r, :] = acc[:, columns] + part

    @pl.loop(0, levels)
    def _(l):
        pltpu.make_async_copy(sb.at[l, others], sb.at[l, others], send_sem.at[l]).wait()

    arrived(4 * reach + 1, one_send)
    arrived(4 * reach - 2, two_send)


def per_device(perturbation, vertical, kappa, sea_mask, sweeps):
    devices = lax.axis_size("gx")
    levels, rows, columns = perturbation.shape
    own = rows // devices
    blocks = columns // LANES
    steps = rows // SUBS
    slot = own * blocks
    total = vertical.shape[0]
    f32 = jnp.float32
    dma = pltpu.SemaphoreType.DMA
    result = pl.pallas_call(
        functools.partial(kernel, devices, levels, rows),
        out_shape=pltpu.VMEM((total, own, columns), f32),
        in_specs=[pl.BlockSpec(memory_space=pl.ANY)] * 5,
        out_specs=pl.BlockSpec(memory_space=pltpu.VMEM),
        scratch_shapes=[
            pltpu.VMEM((levels, blocks, rows, LANES), f32),
            pltpu.VMEM(vertical.shape, f32),
            pltpu.VMEM(kappa.shape, f32),
            pltpu.VMEM(sea_mask.shape, jnp.int32),
            pltpu.SMEM(sweeps.shape, jnp.int32),
            pltpu.VMEM((devices, slot, LANES), f32),
            pltpu.VMEM((5, steps, blocks, SUBS, LANES), f32),
            pltpu.VMEM((levels, steps, blocks, SUBS, LANES), f32),
            pltpu.VMEM((steps, blocks, SUBS, LANES), f32),
            pltpu.VMEM((levels, devices * slot, LANES), f32),
            pltpu.VMEM((levels, devices * slot, LANES), f32),
            pltpu.VMEM((levels, total, 3 * devices), jnp.bfloat16),
            pltpu.VMEM((total, own * columns), f32),
            dma((4 + blocks,)),
            dma(()), dma((3,)), dma(()), dma(()),
            dma((levels,)), dma((levels,)),
        ],
        compiler_params=pltpu.CompilerParams(collective_id=0, has_side_effects=True),
        name="smooth_and_send",
    )(perturbation, vertical, kappa, sea_mask, sweeps)
    return result


def solution(mesh):
    in_specs = (
        P(("member", "gx"), None, None),
        P("member", None),
        P(("member", "gx"), None),
        P("gx", None),
        P("member"),
    )
    out_specs = P("member", "gx", None)
    return jax.shard_map(
        per_device, mesh=mesh, in_specs=in_specs, out_specs=out_specs, check_vma=False
    )
```
